32 devices in a mesh: leaf: 16 (over z, y, x), player: 2 (over core).
Axes of the slice: x: 2, y: 2, z: 4, core: 2. Of those that a mesh axis runs over, the one named last changes fastest.
Arguments:
- chance_reach: float32 [2, 512, 1326], P('player', 'leaf'), may hold values from 0.02 to 1
- regrets_start: float32 [2, 512, 1326], P('player', 'leaf'), may hold values from -6 to 6
- pot: float32 [512], P('leaf'), may hold values from 1 to 8
- parent: int32 [2, 512], P('player'), may hold values from 0 to 255, never falling along the last dimension, each value on 1 to 6 neighbouring positions
- hand_cards: int32 [1326, 2], replicated, may hold values from 0 to 51, as said below
- board_cards: int32 [64, 5], P('leaf'), may hold values from 0 to 51, as said below
- hand_rank: int32 [64, 1326], P('leaf'), may hold values from 0 to 1999
Outputs:
- regrets: float32 [2, 512, 1326], P('player', 'leaf')
- values: float32 [2, 512, 1326], P('player', 'leaf')
The draws below stay inside these ranges and needn't reach their ends.
Inputs may be any that keep to these rules, and one draw needn't show every extreme that they name: `parent`: along each row the node ids never fall; each node owns 1 to 6 consecutive leaves, one exactly 6; every id up to 255 occurs. `hand_cards`: distinct pairs of two different cards, the smaller card first. `board_cards`: five different cards on each board.
All inputs are finite; a program needn't handle non-finite values.
Results may differ from the reference program's by a relative error of at most 0.0003.
Values sent between devices are 32-bit elements; how exact they have to be, the bound alone decides.
A program may use at most 128 MiB of HBM per device.

```python
import math
import jax
import jax.numpy as jnp
import numpy as np
from jax import lax

H = 1326
BOARD_LEAVES = 8
MOST = 6
ITERS = 2
LEAVES = 512
BOARDS = 64
NODES = 256


def draw_hand_cards(key, part):
    lower_cards, upper_cards = np.triu_indices(52, 1)
    card_pairs = jnp.stack([jnp.asarray(lower_cards, jnp.int32), jnp.asarray(upper_cards, jnp.int32)], axis=1)
    chosen = jax.random.permutation(jax.random.fold_in(key, 3), card_pairs.shape[0])[:H]
    return card_pairs[chosen].astype(jnp.int32)


def draw_board_cards(key, part):
    board_keys = jax.random.split(jax.random.fold_in(key, 7), BOARDS)
    return jax.vmap(lambda board_key: jax.random.permutation(board_key, 52)[:5])(board_keys).astype(jnp.int32)


def place_ends(values, rng, least, high):
    longest = values.shape.index(max(values.shape))
    spots = []
    for shift in (0, 1):
        where = [jax.random.randint(jax.random.fold_in(rng, axis), (), 0, length) for axis, length in enumerate(values.shape)]
        where[longest] = (where[longest] + shift) % values.shape[longest]
        spots.append(tuple(where))
    return values.at[spots[0]].set(least).at[spots[1]].set(high)


def levels(rng, shape, cuts, least, top_value):
    factor_of, own = 1.0, jax.random.fold_in(rng, 6)
    for axis_at, blocks in cuts:
        draws = jnp.exp(jax.random.uniform(jax.random.fold_in(own, axis_at), (blocks,), jnp.float32, least / len(cuts), top_value / len(cuts)))
        factor_of = factor_of * jnp.repeat(draws, shape[axis_at] // blocks).reshape([-1 if axis == axis_at else 1 for axis in range(len(shape))])
    return factor_of


def profile(amount, total, limit, skew):
    portions = [(1 << 20) // math.isqrt(standing ** skew) + 1 for standing in range(2, amount + 1)]
    surplus, given = total - limit - (amount - 1), [1] * (amount - 1)
    while surplus > 0:
        movable = [i for i in range(amount - 1) if given[i] < limit]
        mass, budget = sum([portions[i] for i in movable]), surplus
        for i in movable:
            extra = min(limit - given[i], max(1, budget * portions[i] // mass), surplus)
            given[i] = given[i] + extra
            surplus = surplus - extra
    return np.array([limit] + given)


def ragged(key, number_of, total, most, slope):
    if number_of == 2:
        one = jax.random.randint(key, (), max(1, total - most), min(most, total - 1) + 1)
        return jnp.stack([one, total - one])
    lengths = jnp.asarray(profile(number_of, total, most, slope), jnp.int32)
    couples = (number_of - 1) // 2
    source_of, sink = lengths[1:1 + 2 * couples:2], lengths[2:2 + 2 * couples:2]
    room = jnp.minimum(source_of - 1, most - sink)
    shifted = jax.random.randint(jax.random.fold_in(key, 1), (couples,), 0, 1 << 20) % (room + 1)
    lengths = lengths.at[1:1 + 2 * couples:2].set(source_of - shifted).at[2:2 + 2 * couples:2].set(sink + shifted)
    return lengths[jax.random.permutation(jax.random.fold_in(key, 2), number_of)]


def bell_draw(rng, shape, width, bound, cuts=(), kind=jnp.bfloat16):
    factor_of = levels(rng, shape, cuts, -0.22, 0.18) if cuts else 1.0
    values = jax.random.normal(rng, shape, jnp.float32) * width * factor_of
    return jnp.minimum(jnp.maximum(values, -bound), bound).astype(kind)


def setup_inputs(seed: int = 0) -> dict:
    arg_keys = jax.random.split(jax.random.key(seed), 8)
    return {
        "chance_reach": jnp.clip(jnp.exp(math.log(1.0) - 3.912023 * jax.random.uniform(arg_keys[0], (2, LEAVES, H), jnp.float32) ** levels(arg_keys[0], (2, LEAVES, H), ((0, 2), (1, 16)), -0.2, 0.2)), 0.02, 1.0),
        "regrets_start": bell_draw(arg_keys[1], (2, LEAVES, H), 1.0, 6.0, ((0, 2), (1, 16)), jnp.float32),
        "pot": jnp.clip(jnp.exp(math.log(8.0) - 2.0794415 * jax.random.uniform(arg_keys[2], (LEAVES,), jnp.float32) ** levels(arg_keys[2], (LEAVES,), ((0, 16),), -0.2, 0.2)), 1.0, 8.0),
        "parent": jax.vmap(lambda own: jnp.searchsorted(jnp.cumsum(ragged(own, NODES, LEAVES, MOST, 2)), jnp.arange(LEAVES), side="right"))(jax.random.split(arg_keys[3], 2)).reshape((2, LEAVES)).astype(jnp.int32),
        "hand_cards": draw_hand_cards(jax.random.fold_in(arg_keys[7], 71), 0),
        "board_cards": draw_board_cards(jax.random.fold_in(arg_keys[7], 71), 0),
        "hand_rank": place_ends(jax.random.randint(arg_keys[6], (BOARDS, H), 0, 2000), jax.random.fold_in(arg_keys[6], 1), 0, 1999).astype(jnp.int32),
    }


DELTA = 0.05
EPSILON = 1e-06
DECK_SIZE = 52

def holding_table(hand_cards):
    deck_cards = jnp.arange(DECK_SIZE, dtype=jnp.int32)
    holding = (hand_cards[:, 0:1] == deck_cards[None, :]) | (hand_cards[:, 1:2] == deck_cards[None, :])
    return holding.astype(jnp.float32)

def board_free(board_cards, holding):
    deck_cards = jnp.arange(DECK_SIZE, dtype=jnp.int32)
    on_board = jnp.any(board_cards[:, :, None] == deck_cards[None, None, :], axis=1).astype(jnp.float32)
    touched = jnp.dot(on_board, holding.T, precision=lax.Precision.HIGHEST)
    return (touched < 0.5).astype(jnp.float32)

def payoff_matrix(rank_row, free_row, apart_mask):
    ranked = rank_row.astype(jnp.float32)
    sign_table = jnp.sign(ranked[:, None] - ranked[None, :])
    return sign_table * apart_mask * free_row[:, None] * free_row[None, :]

def node_totals(values, parents):
    totals = jax.ops.segment_sum(values, parents, num_segments=NODES)
    return totals[parents]

def reference(chance_reach, regrets_start, pot, parent, hand_cards, board_cards, hand_rank):
    holding = holding_table(hand_cards)
    apart_mask = (jnp.dot(holding, holding.T, precision=lax.Precision.HIGHEST) < 0.5).astype(jnp.float32)
    free_rows = board_free(board_cards, holding)
    pot_rows = pot.reshape(BOARDS, BOARD_LEAVES)
    regrets = regrets_start
    values = jnp.zeros_like(regrets_start)
    for iteration in range(ITERS):
        policy = []
        for player in range(2):
            positive = jnp.maximum(regrets[player], 0.0) + DELTA
            policy.append(positive / node_totals(positive, parent[player]))
        policy = jnp.stack(policy)
        own_reach = chance_reach * policy
        opposed = jnp.stack([own_reach[1], own_reach[0]]).reshape(2, BOARDS, BOARD_LEAVES, H).transpose(1, 0, 2, 3)

        def one_board(board_items):
            rank_row, free_row, opp_block, pot_row = board_items
            matrix = payoff_matrix(rank_row, free_row, apart_mask)
            summed = jnp.einsum('pkg,hg->pkh', opp_block, matrix, precision=lax.Precision.HIGHEST)
            return summed * (pot_row[None, :, None] * (1.0 / H))
        values = lax.map(one_board, (hand_rank, free_rows, opposed, pot_rows))
        values = values.transpose(1, 0, 2, 3).reshape(2, LEAVES, H)
        updated = []
        for player in range(2):
            instant = values[player] - node_totals(policy[player] * values[player], parent[player])
            norm_scale = jnp.sqrt(jnp.sum(instant * instant) / (LEAVES * H) + EPSILON)
            updated.append(regrets[player] + instant / norm_scale)
        regrets = jnp.stack(updated)
    return (regrets, values)
```

```python
import functools

import jax
import jax.numpy as jnp
from jax import lax
from jax.experimental import pallas as pl
from jax.experimental.pallas import tpu as pltpu
from jax.sharding import PartitionSpec as P

ITERS = 2
DELTA = 0.05
EPSILON = 1e-06
DECK_SIZE = 52
LANES = 128
WIDE = 256
SPLIT = 5
MESH = pl.DeviceIdType.MESH
HIGHEST = lax.Precision.HIGHEST
F32 = jnp.float32
BF16 = jnp.bfloat16


def round_up(value, unit):
    return (value + unit - 1) // unit * unit


def column_of(row, count):
    down = lax.broadcasted_iota(jnp.int32, (count, count), 0)
    across = lax.broadcasted_iota(jnp.int32, (count, count), 1)
    return jnp.sum(jnp.where(down == across, row, 0.0), axis=1, keepdims=True)


def row_of(column, count):
    down = lax.broadcasted_iota(jnp.int32, (count, count), 0)
    across = lax.broadcasted_iota(jnp.int32, (count, count), 1)
    return jnp.sum(jnp.where(down == across, column, 0.0), axis=0, keepdims=True)


def kernel(
    n, boards, rows, hands, leaf_count,
    chance, regrets, pot, parent, cards, board_cards, rank,
    out_regrets, out_values,
    payoff, left, right, high, free, cards_wide, rank_wide, pots, same, split,
    held, policy, reach, opposed, values, square_out, square_in,
    held_send, held_recv, value_send, value_recv, reach_send, reach_recv, square_send, square_recv,
):
    me = lax.axis_index("leaf")
    player = lax.axis_index("player")
    before, after = lax.rem(me + n - 1, n), lax.rem(me + 1, n)
    width = payoff.shape[1]
    depth = left.shape[0]
    chunks = boards + 2
    total = chunks * rows

    zeros = jnp.zeros((rows, hands), F32)
    for edge in (0, chunks - 1):
        held[edge] = zeros
        for it in range(ITERS):
            values[it, edge] = zeros

    barrier = pltpu.get_barrier_semaphore()

    def greet(k, carry):
        pl.semaphore_signal(barrier, inc=1, device_id={"leaf": lax.rem(me + k, n)}, device_id_type=MESH)
        return carry

    pl.semaphore_signal(barrier, inc=1, device_id={"player": 1 - player}, device_id_type=MESH)
    lax.fori_loop(1, n, greet, 0)

    cards_wide[...] = jnp.full(cards_wide.shape, -1, jnp.int32)
    cards_wide[:, :hands] = cards[...]
    rank_wide[...] = jnp.zeros(rank_wide.shape, jnp.int32)
    rank_wide[:boards, :hands] = rank[...]
    card = lax.broadcasted_iota(jnp.int32, (depth, width), 0)
    lane = lax.broadcasted_iota(jnp.int32, (depth, width), 1)
    holding = ((card == cards_wide[0:1, :]) | (card == cards_wide[1:2, :])).astype(F32)
    valid = ((card == depth - 1) & (lane < hands)).astype(F32)
    ranked = rank_wide[...]
    code = ((128 + (ranked & 127)) << (ranked >> 7)).astype(F32)
    left[...] = holding + valid
    left[DECK_SIZE : DECK_SIZE + boards, :] = code[:boards]
    right[:, :width] = (valid - holding).astype(BF16)
    pick = lax.broadcasted_iota(jnp.int32, (depth, boards * LANES), 0) - DECK_SIZE
    spot = lax.broadcasted_iota(jnp.int32, (depth, boards * LANES), 1)
    right[:, width:] = ((spot >= pick * LANES) & (spot < pick * LANES + LANES)).astype(BF16)
    for b in range(boards):
        high[b] = jnp.broadcast_to(code[b : b + 1], (16, width)).astype(BF16)
    deck = lax.broadcasted_iota(jnp.int32, (boards, depth), 1)
    on_board = jnp.zeros((boards, depth), jnp.bool_)
    for k in range(board_cards.shape[1]):
        on_board = on_board | (deck == board_cards[:, k : k + 1])
    touched = jnp.dot(on_board.astype(BF16), holding.astype(BF16), preferred_element_type=F32)
    free[...] = (touched < 0.5).astype(F32)

    def build(i, carry):
        start = pl.multiple_of(i * LANES, LANES)
        down = left[:, pl.ds(start, LANES)].T.astype(BF16)
        lows = jnp.dot(down, right[:, width:], preferred_element_type=F32).astype(BF16)
        for first in range(0, width, WIDE):
            last = min(first + WIDE, width)
            apart = jnp.dot(down, right[:, first:last], preferred_element_type=F32)
            apart = jnp.maximum(apart, 0.0).astype(BF16)
            for at in range(first, last, LANES):
                bound = apart[:, at - first : at - first + LANES].reshape(LANES // 16, 16, LANES)
                for b in range(boards):
                    low = lows[:, b * LANES : (b + 1) * LANES].reshape(LANES // 16, 16, LANES)
                    gap = high[b, :, at : at + LANES][None] - low
                    entry = jnp.minimum(jnp.maximum(gap, -bound), bound)
                    payoff[b, pl.ds(start, LANES), at : at + LANES] = entry.reshape(LANES, LANES)
        return carry

    blocks = width // LANES
    lax.fori_loop(0, SPLIT, build, 0)

    pl.semaphore_wait(barrier, n)

    def to_before(source, target, send, recv):
        return pltpu.make_async_remote_copy(
            src_ref=source, dst_ref=target, send_sem=send, recv_sem=recv,
            device_id={"leaf": before}, device_id_type=MESH)

    def to_after(source, target, send, recv):
        return pltpu.make_async_remote_copy(
            src_ref=source, dst_ref=target, send_sem=send, recv_sem=recv,
            device_id={"leaf": after}, device_id_type=MESH)

    held_down = to_before(regrets.at[0, pl.ds(0, rows)], held.at[chunks - 1], held_send.at[0], held_recv.at[0])
    held_up = to_after(
        regrets.at[0, pl.ds((boards - 1) * rows, rows)], held.at[0], held_send.at[1], held_recv.at[1])
    value_down = [
        to_before(values.at[it, 1], values.at[it, chunks - 1], value_send.at[it, 0], value_recv.at[it, 0])
        for it in range(ITERS)]
    value_up = [
        to_after(values.at[it, boards], values.at[it, 0], value_send.at[it, 1], value_recv.at[it, 1])
        for it in range(ITERS)]

    @pl.when(me > 0)
    def _():
        held_down.start()

    @pl.when(me < n - 1)
    def _():
        held_up.start()

    leaf = me * (boards * rows) - rows + lax.broadcasted_iota(jnp.int32, (total, leaf_count), 0)
    here = lax.broadcasted_iota(jnp.int32, (total, leaf_count), 1)
    ids = jnp.sum(jnp.where(leaf == here, parent[...].astype(F32) + 1.0, 0.0), axis=1, keepdims=True)
    same[...] = (ids == row_of(ids, total)).astype(F32)
    pots[...] = jnp.broadcast_to(
        column_of(pot[...], boards * rows) * (1.0 / hands), (boards * rows, LANES)).reshape(boards, rows, LANES)
    split[...] = jnp.zeros(split.shape, BF16)
    for b in range(boards):
        held[b + 1] = regrets[0, pl.ds(b * rows, rows)]

    lax.fori_loop(SPLIT, blocks, build, 0)

    def node_totals(array):
        return jnp.dot(same[...], array, precision=HIGHEST, preferred_element_type=F32)

    @pl.when(me > 0)
    def _():
        held_up.wait_recv()

    @pl.when(me < n - 1)
    def _():
        held_down.wait_recv()

    standing = held[...].reshape(total, hands)
    for it in range(ITERS):
        positive = jnp.maximum(standing, 0.0) + DELTA
        policy[it] = positive / node_totals(positive)
        own_policy = policy[it, rows : rows + boards * rows]
        reach[it] = (chance[0] * own_policy).reshape(boards, rows, hands)

        def exchange(b, it=it):
            return pltpu.make_async_remote_copy(
                src_ref=reach.at[it, b], dst_ref=opposed.at[it, b],
                send_sem=reach_send.at[it, b], recv_sem=reach_recv.at[it, b],
                device_id={"player": 1 - player}, device_id_type=MESH)

        for t in range(boards):
            exchange(t * (boards - 1) % boards).start()

        def showdown(t, carry, it=it, exchange=exchange):
            b = lax.rem(t * (boards - 1), boards)
            exchange(b).wait_recv()
            open_hands = free[pl.ds(b, 1), :]
            facing = opposed[it, b] * open_hands[:, :hands]
            coarse = facing.astype(BF16).astype(F32)
            split[:, :hands] = jnp.concatenate([coarse, facing - coarse], axis=0).astype(BF16)
            summed = jnp.dot(split[...], payoff[b], preferred_element_type=F32)
            summed = (summed[:rows] + summed[rows:]) * open_hands * pots[b][:, :1]
            values[it, b + 1] = summed[:, :hands]

            @pl.when((t == 0) & (me > 0))
            def _():
                value_down[it].start()

            @pl.when((t == 1) & (me < n - 1))
            def _():
                value_up[it].start()

            return carry

        lax.fori_loop(0, boards, showdown, 0)

        @pl.when(me > 0)
        def _(it=it):
            value_up[it].wait_recv()

        @pl.when(me < n - 1)
        def _(it=it):
            value_down[it].wait_recv()

        gained = values[it].reshape(total, hands)
        instant = gained - node_totals(policy[it] * gained)
        own = instant[rows : rows + boards * rows]
        squares = jnp.sum(jnp.sum(own * own, axis=0, keepdims=True), axis=1, keepdims=True)
        square_out[it] = jnp.broadcast_to(squares, (1, LANES))

        def tell(k, carry, it=it):
            pltpu.make_async_remote_copy(
                src_ref=square_out.at[it], dst_ref=square_in.at[it, k - 1],
                send_sem=square_send.at[it], recv_sem=square_recv.at[it],
                device_id={"leaf": lax.rem(me + k, n)}, device_id_type=MESH).start()
            return carry

        lax.fori_loop(1, n, tell, 0)
        if it == ITERS - 1:
            out_values[0] = gained[rows : rows + boards * rows]
        everyone = square_in.at[it]
        pltpu.make_async_copy(everyone, everyone, square_recv.at[it]).wait()
        squares = square_out[it] + jnp.sum(square_in[it], axis=0)
        inverse = 1.0 / jnp.sqrt(squares[:, :1] / (leaf_count * hands) + EPSILON)
        if it < ITERS - 1:
            standing = standing + instant * inverse
        else:
            out_regrets[0] = standing[rows : rows + boards * rows] + own * inverse

    @pl.when(me > 0)
    def _():
        held_down.wait_send()
        for it in range(ITERS):
            value_down[it].wait_send()

    @pl.when(me < n - 1)
    def _():
        held_up.wait_send()
        for it in range(ITERS):
            value_up[it].wait_send()

    for it in range(ITERS):
        everyone = square_in.at[it]
        pltpu.make_async_copy(everyone, everyone, square_send.at[it]).wait()
        for b in range(boards):
            pltpu.make_async_copy(reach.at[it, b], reach.at[it, b], reach_send.at[it, b]).wait()


def solution(mesh):
    n = mesh.shape["leaf"]

    def local(chance_reach, regrets_start, pot, parent, hand_cards, board_cards, hand_rank):
        leaf_rows, hands = chance_reach.shape[1:]
        boards = hand_rank.shape[0]
        rows = leaf_rows // boards
        leaf_count = parent.shape[1]
        width = round_up(hands, LANES)
        depth = round_up(DECK_SIZE + boards + 1, 16)
        chunks = boards + 2
        vmem = pl.BlockSpec(memory_space=pltpu.VMEM)
        shape = jax.ShapeDtypeStruct(chance_reach.shape, F32)
        dma = pltpu.SemaphoreType.DMA
        return pl.pallas_call(
            functools.partial(kernel, n, boards, rows, hands, leaf_count),
            out_shape=(shape, shape),
            in_specs=[vmem] * 7,
            out_specs=(vmem, vmem),
            scratch_shapes=[
                pltpu.VMEM((boards, width, width), BF16),
                pltpu.VMEM((depth, width), F32),
                pltpu.VMEM((depth, width + boards * LANES), BF16),
                pltpu.VMEM((boards, 16, width), BF16),
                pltpu.VMEM((boards, width), F32),
                pltpu.VMEM((2, width), jnp.int32),
                pltpu.VMEM((round_up(boards, 8), width), jnp.int32),
                pltpu.VMEM((boards, rows, LANES), F32),
                pltpu.VMEM((chunks * rows, chunks * rows), F32),
                pltpu.VMEM((2 * rows, width), BF16),
                pltpu.VMEM((chunks, rows, hands), F32),
                pltpu.VMEM((ITERS, chunks * rows, hands), F32),
                pltpu.VMEM((ITERS, boards, rows, hands), F32),
                pltpu.VMEM((ITERS, boards, rows, hands), F32),
                pltpu.VMEM((ITERS, chunks, rows, hands), F32),
                pltpu.VMEM((ITERS, 1, LANES), F32),
                pltpu.VMEM((ITERS, n - 1, 1, LANES), F32),
                dma((2,)), dma((2,)),
                dma((ITERS, 2)), dma((ITERS, 2)),
                dma((ITERS, boards)), dma((ITERS, boards)),
                dma((ITERS,)), dma((ITERS,)),
            ],
            compiler_params=pltpu.CompilerParams(collective_id=0, has_side_effects=True),
            name="regret",
        )(chance_reach, regrets_start, pot[None], parent, hand_cards.T, board_cards, hand_rank)

    in_specs = (
        P("player", "leaf", None),
        P("player", "leaf", None),
        P("leaf"),
        P("player", None),
        P(),
        P("leaf", None),
        P("leaf", None),
    )
    out_specs = (P("player", "leaf", None), P("player", "leaf", None))
    return jax.shard_map(local, mesh=mesh, in_specs=in_specs, out_specs=out_specs, check_vma=False)
```

```python
import functools

import jax
import jax.numpy as jnp
from jax import lax
from jax.experimental import pallas as pl
from jax.experimental.pallas import tpu as pltpu
from jax.sharding import PartitionSpec as P

ITERS = 2
DELTA = 0.05
EPSILON = 1e-06
DECK_SIZE = 52
LANES = 128
WIDE = 256
SPLIT = 5
MESH = pl.DeviceIdType.MESH
F32 = jnp.float32
BF16 = jnp.bfloat16


def round_up(value, unit):
    return (value + unit - 1) // unit * unit


def column_of(row, count):
    down = lax.broadcasted_iota(jnp.int32, (count, count), 0)
    across = lax.broadcasted_iota(jnp.int32, (count, count), 1)
    return jnp.sum(jnp.where(down == across, row, 0.0), axis=1, keepdims=True)


def row_of(column, count):
    down = lax.broadcasted_iota(jnp.int32, (count, count), 0)
    across = lax.broadcasted_iota(jnp.int32, (count, count), 1)
    return jnp.sum(jnp.where(down == across, column, 0.0), axis=0, keepdims=True)


def kernel(
    n, boards, rows, hands, leaf_count,
    chance_far, regrets_far, pot_far, parent_far, cards_far, board_cards_far, rank_far,
    out_regrets, out_values,
    chance, regrets, pot, parent, cards, board_cards, rank, load,
    payoff, left, right, high, lows, free, cards_wide, rank_wide, pots, same, split,
    held, policy, reach, opposed, values, square_out, square_in,
    held_send, held_recv, value_send, value_recv, reach_send, reach_recv, square_send, square_recv,
):
    me = lax.axis_index("leaf")
    player = lax.axis_index("player")
    before, after = lax.rem(me + n - 1, n), lax.rem(me + 1, n)
    width = payoff.shape[1]
    depth = left.shape[0]
    chunks = boards + 2
    total = chunks * rows

    loads = [
        pltpu.make_async_copy(far, near, load.at[i])
        for i, (far, near) in enumerate((
            (cards_far, cards), (board_cards_far, board_cards), (rank_far, rank), (regrets_far, regrets),
            (pot_far, pot), (parent_far, parent), (chance_far, chance)))]
    for copy in loads:
        copy.start()

    zeros = jnp.zeros((rows, hands), F32)
    for edge in (0, chunks - 1):
        held[edge] = zeros
        for it in range(ITERS):
            values[it, edge] = zeros

    barrier = pltpu.get_barrier_semaphore()

    def greet(k, carry):
        pl.semaphore_signal(barrier, inc=1, device_id={"leaf": lax.rem(me + k, n)}, device_id_type=MESH)
        return carry

    pl.semaphore_signal(barrier, inc=1, device_id={"player": 1 - player}, device_id_type=MESH)
    lax.fori_loop(1, n, greet, 0)

    for copy in loads[:3]:
        copy.wait()

    cards_wide[...] = jnp.full(cards_wide.shape, -1, jnp.int32)
    cards_wide[:, :hands] = cards[...]
    rank_wide[...] = jnp.zeros(rank_wide.shape, jnp.int32)
    rank_wide[:boards, :hands] = rank[...]
    card = lax.broadcasted_iota(jnp.int32, (depth, width), 0)
    lane = lax.broadcasted_iota(jnp.int32, (depth, width), 1)
    holding = ((card == cards_wide[0:1, :]) | (card == cards_wide[1:2, :])).astype(F32)
    valid = ((card == depth - 1) & (lane < hands)).astype(F32)
    ranked = rank_wide[...]
    code = ((128 + (ranked & 127)) << (ranked >> 7)).astype(F32)
    left[...] = holding + valid
    left[DECK_SIZE : DECK_SIZE + boards, :] = code[:boards]
    right[:, :width] = (valid - holding).astype(BF16)
    pick = lax.broadcasted_iota(jnp.int32, (depth, boards * LANES), 0) - DECK_SIZE
    spot = lax.broadcasted_iota(jnp.int32, (depth, boards * LANES), 1)
    right[:, width:] = ((spot >= pick * LANES) & (spot < pick * LANES + LANES)).astype(BF16)
    for b in range(boards):
        high[b] = jnp.broadcast_to(code[b : b + 1], (16, width)).astype(BF16)
    deck = lax.broadcasted_iota(jnp.int32, (boards, depth), 1)
    on_board = jnp.zeros((boards, depth), jnp.bool_)
    for k in range(board_cards.shape[1]):
        on_board = on_board | (deck == board_cards[:, k : k + 1])
    touched = jnp.dot(on_board.astype(BF16), holding.astype(BF16), preferred_element_type=F32)
    free[...] = (touched < 0.5).astype(F32)

    def build(i, carry):
        start = pl.multiple_of(i * LANES, LANES)
        down = left[:, pl.ds(start, LANES)].T.astype(BF16)
        coded = jnp.dot(down, right[:, width:], preferred_element_type=F32).astype(BF16)
        for b in range(boards):
            lows[b] = coded[:, b * LANES : (b + 1) * LANES]
        for first in range(0, width, WIDE):
            last = min(first + WIDE, width)
            apart = jnp.dot(down, right[:, first:last], preferred_element_type=F32)
            apart = jnp.maximum(apart.astype(BF16), 0.0)
            for at in range(first, last, LANES):
                for r in range(0, LANES, 16):
                    bound = apart[r : r + 16, at - first : at - first + LANES]
                    floor = -bound
                    for b in range(boards):
                        gap = high[b, :, at : at + LANES] - lows[b, r : r + 16]
                        payoff[b, pl.ds(start + r, 16), at : at + LANES] = jnp.minimum(
                            jnp.maximum(gap, floor), bound)
        return carry

    blocks = width // LANES
    lax.fori_loop(0, SPLIT, build, 0)

    for copy in loads[3:]:
        copy.wait()
    pl.semaphore_wait(barrier, n)

    def to_before(source, target, send, recv):
        return pltpu.make_async_remote_copy(
            src_ref=source, dst_ref=target, send_sem=send, recv_sem=recv,
            device_id={"leaf": before}, device_id_type=MESH)

    def to_after(source, target, send, recv):
        return pltpu.make_async_remote_copy(
            src_ref=source, dst_ref=target, send_sem=send, recv_sem=recv,
            device_id={"leaf": after}, device_id_type=MESH)

    held_down = to_before(regrets.at[0, pl.ds(0, rows)], held.at[chunks - 1], held_send.at[0], held_recv.at[0])
    held_up = to_after(
        regrets.at[0, pl.ds((boards - 1) * rows, rows)], held.at[0], held_send.at[1], held_recv.at[1])
    value_down = [
        to_before(values.at[it, 1], values.at[it, chunks - 1], value_send.at[it, 0], value_recv.at[it, 0])
        for it in range(ITERS)]
    value_up = [
        to_after(values.at[it, boards], values.at[it, 0], value_send.at[it, 1], value_recv.at[it, 1])
        for it in range(ITERS)]

    @pl.when(me > 0)
    def _():
        held_down.start()

    @pl.when(me < n - 1)
    def _():
        held_up.start()

    twice = lax.broadcasted_iota(jnp.int32, (2 * total, leaf_count), 0)
    leaf = me * (boards * rows) - rows + jnp.where(twice >= total, twice - total, twice)
    here = lax.broadcasted_iota(jnp.int32, (2 * total, leaf_count), 1)
    ids = jnp.sum(jnp.where(leaf == here, parent[...].astype(F32) + 1.0, 0.0), axis=1, keepdims=True)
    same[...] = (ids[:total] == row_of(ids, 2 * total)).astype(BF16)
    pots[...] = jnp.broadcast_to(
        column_of(pot[...], boards * rows) * (1.0 / hands), (boards * rows, LANES)).reshape(boards, rows, LANES)
    split[...] = jnp.zeros(split.shape, BF16)
    for b in range(boards):
        held[b + 1] = regrets[0, pl.ds(b * rows, rows)]

    lax.fori_loop(SPLIT, blocks, build, 0)

    def node_totals(array):
        coarse = array.astype(BF16)
        fine = (array - coarse.astype(F32)).astype(BF16)
        return jnp.dot(same[...], jnp.concatenate([coarse, fine], axis=0), preferred_element_type=F32)

    @pl.when(me > 0)
    def _():
        held_up.wait_recv()

    @pl.when(me < n - 1)
    def _():
        held_down.wait_recv()

    standing = held[...].reshape(total, hands)
    for it in range(ITERS):
        positive = jnp.maximum(standing, 0.0) + DELTA
        policy[it] = positive / node_totals(positive)
        own_policy = policy[it, rows : rows + boards * rows]
        reach[it] = (chance[0] * own_policy).reshape(boards, rows, hands)

        def exchange(b, it=it):
            return pltpu.make_async_remote_copy(
                src_ref=reach.at[it, b], dst_ref=opposed.at[it, b],
                send_sem=reach_send.at[it, b], recv_sem=reach_recv.at[it, b],
                device_id={"player": 1 - player}, device_id_type=MESH)

        for t in range(boards):
            exchange(t * (boards - 1) % boards).start()

        def showdown(t, carry, it=it, exchange=exchange):
            b = lax.rem(t * (boards - 1), boards)
            exchange(b).wait_recv()
            open_hands = free[pl.ds(b, 1), :]
            facing = opposed[it, b] * open_hands[:, :hands]
            coarse = facing.astype(BF16).astype(F32)
            split[:, :hands] = jnp.concatenate([coarse, facing - coarse], axis=0).astype(BF16)
            summed = jnp.dot(split[...], payoff[b], preferred_element_type=F32)
            summed = (summed[:rows] + summed[rows:]) * open_hands * pots[b][:, :1]
            values[it, b + 1] = summed[:, :hands]

            @pl.when((t == 0) & (me > 0))
            def _():
                value_down[it].start()

            @pl.when((t == 1) & (me < n - 1))
            def _():
                value_up[it].start()

            return carry

        lax.fori_loop(0, boards, showdown, 0)

        @pl.when(me > 0)
        def _(it=it):
            value_up[it].wait_recv()

        @pl.when(me < n - 1)
        def _(it=it):
            value_down[it].wait_recv()

        gained = values[it].reshape(total, hands)
        instant = gained - node_totals(policy[it] * gained)
        own = instant[rows : rows + boards * rows]
        squares = jnp.sum(jnp.sum(own * own, axis=0, keepdims=True), axis=1, keepdims=True)
        square_out[it] = jnp.broadcast_to(squares, (1, LANES))

        def tell(k, carry, it=it):
            pltpu.make_async_remote_copy(
                src_ref=square_out.at[it], dst_ref=square_in.at[it, k - 1],
                send_sem=square_send.at[it], recv_sem=square_recv.at[it],
                device_id={"leaf": lax.rem(me + k, n)}, device_id_type=MESH).start()
            return carry

        lax.fori_loop(1, n, tell, 0)
        if it == ITERS - 1:
            out_values[0] = gained[rows : rows + boards * rows]
        everyone = square_in.at[it]
        pltpu.make_async_copy(everyone, everyone, square_recv.at[it]).wait()
        squares = square_out[it] + jnp.sum(square_in[it], axis=0)
        inverse = 1.0 / jnp.sqrt(squares[:, :1] / (leaf_count * hands) + EPSILON)
        if it < ITERS - 1:
            standing = standing + instant * inverse
        else:
            out_regrets[0] = standing[rows : rows + boards * rows] + own * inverse

    @pl.when(me > 0)
    def _():
        held_down.wait_send()
        for it in range(ITERS):
            value_down[it].wait_send()

    @pl.when(me < n - 1)
    def _():
        held_up.wait_send()
        for it in range(ITERS):
            value_up[it].wait_send()

    for it in range(ITERS):
        everyone = square_in.at[it]
        pltpu.make_async_copy(everyone, everyone, square_send.at[it]).wait()
        for b in range(boards):
            pltpu.make_async_copy(reach.at[it, b], reach.at[it, b], reach_send.at[it, b]).wait()


def solution(mesh):
    n = mesh.shape["leaf"]

    def local(chance_reach, regrets_start, pot, parent, hand_cards, board_cards, hand_rank):
        leaf_rows, hands = chance_reach.shape[1:]
        boards = hand_rank.shape[0]
        rows = leaf_rows // boards
        leaf_count = parent.shape[1]
        width = round_up(hands, LANES)
        depth = round_up(DECK_SIZE + boards + 1, 16)
        chunks = boards + 2
        vmem = pl.BlockSpec(memory_space=pltpu.VMEM)
        shape = pltpu.VMEM(chance_reach.shape, F32)
        dma = pltpu.SemaphoreType.DMA
        arrays = (chance_reach, regrets_start, pot[None], parent, hand_cards.T, board_cards, hand_rank)
        return pl.pallas_call(
            functools.partial(kernel, n, boards, rows, hands, leaf_count),
            out_shape=(shape, shape),
            in_specs=[pl.BlockSpec(memory_space=pl.ANY)] * len(arrays),
            out_specs=(vmem, vmem),
            scratch_shapes=[
                *(pltpu.VMEM(array.shape, array.dtype) for array in arrays),
                pltpu.SemaphoreType.DMA((len(arrays),)),
                pltpu.VMEM((boards, width, width), BF16),
                pltpu.VMEM((depth, width), F32),
                pltpu.VMEM((depth, width + boards * LANES), BF16),
                pltpu.VMEM((boards, 16, width), BF16),
                pltpu.VMEM((boards, LANES, LANES), BF16),
                pltpu.VMEM((boards, width), F32),
                pltpu.VMEM((2, width), jnp.int32),
                pltpu.VMEM((round_up(boards, 8), width), jnp.int32),
                pltpu.VMEM((boards, rows, LANES), F32),
                pltpu.VMEM((chunks * rows, 2 * chunks * rows), BF16),
                pltpu.VMEM((2 * rows, width), BF16),
                pltpu.VMEM((chunks, rows, hands), F32),
                pltpu.VMEM((ITERS, chunks * rows, hands), F32),
                pltpu.VMEM((ITERS, boards, rows, hands), F32),
                pltpu.VMEM((ITERS, boards, rows, hands), F32),
                pltpu.VMEM((ITERS, chunks, rows, hands), F32),
                pltpu.VMEM((ITERS, 1, LANES), F32),
                pltpu.VMEM((ITERS, n - 1, 1, LANES), F32),
                dma((2,)), dma((2,)),
                dma((ITERS, 2)), dma((ITERS, 2)),
                dma((ITERS, boards)), dma((ITERS, boards)),
                dma((ITERS,)), dma((ITERS,)),
            ],
            compiler_params=pltpu.CompilerParams(collective_id=0, has_side_effects=True),
            name="regret",
        )(*arrays)

    in_specs = (
        P("player", "leaf", None),
        P("player", "leaf", None),
        P("leaf"),
        P("player", None),
        P(),
        P("leaf", None),
        P("leaf", None),
    )
    out_specs = (P("player", "leaf", None), P("player", "leaf", None))
    return jax.shard_map(local, mesh=mesh, in_specs=in_specs, out_specs=out_specs, check_vma=False)
```

```python
import functools

import jax
import jax.numpy as jnp
from jax import lax
from jax.experimental import pallas as pl
from jax.experimental.pallas import tpu as pltpu
from jax.sharding import PartitionSpec as P

ITERS = 2
MOST = 6
DELTA = 0.05
EPSILON = 1e-06
DECK_SIZE = 52
LANES = 128
WIDE = 256
SPLIT = 5
MESH = pl.DeviceIdType.MESH
F32 = jnp.float32
BF16 = jnp.bfloat16


def round_up(value, unit):
    return (value + unit - 1) // unit * unit


def column_of(row, count):
    down = lax.broadcasted_iota(jnp.int32, (count, count), 0)
    across = lax.broadcasted_iota(jnp.int32, (count, count), 1)
    return jnp.sum(jnp.where(down == across, row, 0.0), axis=1, keepdims=True)


def row_of(column, count):
    down = lax.broadcasted_iota(jnp.int32, (count, count), 0)
    across = lax.broadcasted_iota(jnp.int32, (count, count), 1)
    return jnp.sum(jnp.where(down == across, column, 0.0), axis=0, keepdims=True)


def kernel(
    n, boards, rows, hands, leaf_count,
    chance_far, regrets_far, pot_far, parent_far, cards_far, board_cards_far, rank_far,
    out_regrets, out_values,
    chance, regrets, pot, parent, cards, board_cards, rank, load,
    payoff, left, right, free, cards_wide, rank_wide, pots, same, split,
    held, policy, reach, opposed, values, square_out, square_in,
    held_send, held_recv, value_send, value_recv, reach_send, reach_recv, square_send, square_recv,
):
    me = lax.axis_index("leaf")
    player = lax.axis_index("player")
    before, after = lax.rem(me + n - 1, n), lax.rem(me + 1, n)
    width = payoff.shape[1]
    depth = left.shape[0]
    chunks = boards + 2
    total = chunks * rows

    loads = [
        pltpu.make_async_copy(far, near, load.at[i])
        for i, (far, near) in enumerate((
            (cards_far, cards), (board_cards_far, board_cards), (rank_far, rank), (regrets_far, regrets),
            (pot_far, pot), (parent_far, parent), (chance_far, chance)))]
    for copy in loads:
        copy.start()

    zeros = jnp.zeros((rows, hands), F32)
    for edge in (0, chunks - 1):
        held[edge] = zeros
        for it in range(ITERS):
            values[it, edge] = zeros

    barrier = pltpu.get_barrier_semaphore()

    def greet(k, carry):
        pl.semaphore_signal(barrier, inc=1, device_id={"leaf": lax.rem(me + k, n)}, device_id_type=MESH)
        return carry

    pl.semaphore_signal(barrier, inc=1, device_id={"player": 1 - player}, device_id_type=MESH)
    lax.fori_loop(1, n, greet, 0)

    for copy in loads[:3]:
        copy.wait()

    cards_wide[...] = jnp.full(cards_wide.shape, -1, jnp.int32)
    cards_wide[:, :hands] = cards[...]
    rank_wide[...] = jnp.zeros(rank_wide.shape, jnp.int32)
    rank_wide[:boards, :hands] = rank[...]
    card = lax.broadcasted_iota(jnp.int32, (depth, width), 0)
    lane = lax.broadcasted_iota(jnp.int32, (depth, width), 1)
    holding = ((card == cards_wide[0:1, :]) | (card == cards_wide[1:2, :])).astype(F32)
    valid = ((card == depth - 1) & (lane < hands)).astype(F32)
    ranked = rank_wide[...]
    code = ((128 + (ranked & 127)) << (ranked >> 7)).astype(F32)
    left[...] = holding + valid
    left[DECK_SIZE : DECK_SIZE + boards, :] = code[:boards]
    right[:, :width] = (valid - holding).astype(BF16)
    pick = lax.broadcasted_iota(jnp.int32, (depth, boards * LANES), 0) - DECK_SIZE
    spot = lax.broadcasted_iota(jnp.int32, (depth, boards * LANES), 1)
    right[:, width:] = ((spot >= pick * LANES) & (spot < pick * LANES + LANES)).astype(BF16)
    deck = lax.broadcasted_iota(jnp.int32, (boards, depth), 1)
    on_board = jnp.zeros((boards, depth), jnp.bool_)
    for k in range(board_cards.shape[1]):
        on_board = on_board | (deck == board_cards[:, k : k + 1])
    touched = jnp.dot(on_board.astype(BF16), holding.astype(BF16), preferred_element_type=F32)
    free[...] = (touched < 0.5).astype(F32)

    def build(i, carry):
        start = pl.multiple_of(i * LANES, LANES)
        down = left[:, pl.ds(start, LANES)].T.astype(BF16)
        lows = jnp.dot(down, right[:, width:], preferred_element_type=F32).astype(BF16)
        for first in range(0, width, WIDE):
            last = min(first + WIDE, width)
            apart = jnp.dot(down, right[:, first:last], preferred_element_type=F32)
            apart = jnp.maximum(apart.astype(BF16), 0.0)
            for at in range(first, last, LANES):
                highs = [
                    jnp.broadcast_to(left[DECK_SIZE + b : DECK_SIZE + b + 1, at : at + LANES], (16, LANES)).astype(BF16)
                    for b in range(boards)]
                for r in range(0, LANES, 16):
                    bound = apart[r : r + 16, at - first : at - first + LANES]
                    floor = -bound
                    for b in range(boards):
                        gap = highs[b] - lows[r : r + 16, b * LANES : (b + 1) * LANES]
                        payoff[b, pl.ds(start + r, 16), at : at + LANES] = jnp.minimum(
                            jnp.maximum(gap, floor), bound)
        return carry

    blocks = width // LANES
    lax.fori_loop(0, SPLIT, build, 0)

    for copy in loads[3:]:
        copy.wait()
    pl.semaphore_wait(barrier, n)

    def to_before(source, target, send, recv):
        return pltpu.make_async_remote_copy(
            src_ref=source, dst_ref=target, send_sem=send, recv_sem=recv,
            device_id={"leaf": before}, device_id_type=MESH)

    def to_after(source, target, send, recv):
        return pltpu.make_async_remote_copy(
            src_ref=source, dst_ref=target, send_sem=send, recv_sem=recv,
            device_id={"leaf": after}, device_id_type=MESH)

    reach_of = min(MOST - 1, rows)
    held_down = to_before(
        regrets.at[0, pl.ds(0, reach_of)], held.at[chunks - 1, pl.ds(0, reach_of)], held_send.at[0], held_recv.at[0])
    held_up = to_after(
        regrets.at[0, pl.ds(boards * rows - reach_of, reach_of)], held.at[0, pl.ds(rows - reach_of, reach_of)], held_send.at[1], held_recv.at[1])
    value_down = [
        to_before(
            values.at[it, 1, pl.ds(0, reach_of)], values.at[it, chunks - 1, pl.ds(0, reach_of)], value_send.at[it, 0], value_recv.at[it, 0])
        for it in range(ITERS)]
    value_up = [
        to_after(
            values.at[it, boards, pl.ds(rows - reach_of, reach_of)], values.at[it, 0, pl.ds(rows - reach_of, reach_of)],
            value_send.at[it, 1], value_recv.at[it, 1])
        for it in range(ITERS)]

    @pl.when(me > 0)
    def _():
        held_down.start()

    @pl.when(me < n - 1)
    def _():
        held_up.start()

    twice = lax.broadcasted_iota(jnp.int32, (2 * total, leaf_count), 0)
    leaf = me * (boards * rows) - rows + jnp.where(twice >= total, twice - total, twice)
    here = lax.broadcasted_iota(jnp.int32, (2 * total, leaf_count), 1)
    ids = jnp.sum(jnp.where(leaf == here, parent[...].astype(F32) + 1.0, 0.0), axis=1, keepdims=True)
    same[...] = (ids[:total] == row_of(ids, 2 * total)).astype(BF16)
    pots[...] = jnp.broadcast_to(
        column_of(pot[...], boards * rows) * (1.0 / hands), (boards * rows, LANES)).reshape(boards, rows, LANES)
    split[...] = jnp.zeros(split.shape, BF16)
    for b in range(boards):
        held[b + 1] = regrets[0, pl.ds(b * rows, rows)]

    lax.fori_loop(SPLIT, blocks, build, 0)

    def node_totals(array):
        coarse = array.astype(BF16)
        fine = (array - coarse.astype(F32)).astype(BF16)
        return jnp.dot(same[...], jnp.concatenate([coarse, fine], axis=0), preferred_element_type=F32)

    @pl.when(me > 0)
    def _():
        held_up.wait_recv()

    @pl.when(me < n - 1)
    def _():
        held_down.wait_recv()

    standing = held[...].reshape(total, hands)
    for it in range(ITERS):
        positive = jnp.maximum(standing, 0.0) + DELTA
        policy[it] = positive / node_totals(positive)
        own_policy = policy[it, rows : rows + boards * rows]
        reach[it] = (chance[0] * own_policy).reshape(boards, rows, hands)

        def exchange(b, it=it):
            return pltpu.make_async_remote_copy(
                src_ref=reach.at[it, b], dst_ref=opposed.at[it, b],
                send_sem=reach_send.at[it, b], recv_sem=reach_recv.at[it, b],
                device_id={"player": 1 - player}, device_id_type=MESH)

        for t in range(boards):
            exchange(t * (boards - 1) % boards).start()

        def showdown(t, carry, it=it, exchange=exchange):
            b = lax.rem(t * (boards - 1), boards)
            exchange(b).wait_recv()
            open_hands = free[pl.ds(b, 1), :]
            facing = opposed[it, b] * open_hands[:, :hands]
            coarse = facing.astype(BF16).astype(F32)
            split[:, :hands] = jnp.concatenate([coarse, facing - coarse], axis=0).astype(BF16)
            summed = jnp.dot(split[...], payoff[b], preferred_element_type=F32)
            summed = (summed[:rows] + summed[rows:]) * open_hands * pots[b][:, :1]
            values[it, b + 1] = summed[:, :hands]

            @pl.when((t == 0) & (me > 0))
            def _():
                value_down[it].start()

            @pl.when((t == 1) & (me < n - 1))
            def _():
                value_up[it].start()

            return carry

        lax.fori_loop(0, boards, showdown, 0)

        @pl.when(me > 0)
        def _(it=it):
            value_up[it].wait_recv()

        @pl.when(me < n - 1)
        def _(it=it):
            value_down[it].wait_recv()

        gained = values[it].reshape(total, hands)
        instant = gained - node_totals(policy[it] * gained)
        own = instant[rows : rows + boards * rows]
        squares = jnp.sum(jnp.sum(own * own, axis=0, keepdims=True), axis=1, keepdims=True)
        square_out[it] = jnp.broadcast_to(squares, (1, LANES))

        def tell(k, carry, it=it):
            pltpu.make_async_remote_copy(
                src_ref=square_out.at[it], dst_ref=square_in.at[it, k - 1],
                send_sem=square_send.at[it], recv_sem=square_recv.at[it],
                device_id={"leaf": lax.rem(me + k, n)}, device_id_type=MESH).start()
            return carry

        lax.fori_loop(1, n, tell, 0)
        if it == ITERS - 1:
            out_values[0] = gained[rows : rows + boards * rows]
        everyone = square_in.at[it]
        pltpu.make_async_copy(everyone, everyone, square_recv.at[it]).wait()
        squares = square_out[it] + jnp.sum(square_in[it], axis=0)
        inverse = 1.0 / jnp.sqrt(squares[:, :1] / (leaf_count * hands) + EPSILON)
        if it < ITERS - 1:
            standing = standing + instant * inverse
        else:
            out_regrets[0] = standing[rows : rows + boards * rows] + own * inverse

    @pl.when(me > 0)
    def _():
        held_down.wait_send()
        for it in range(ITERS):
            value_down[it].wait_send()

    @pl.when(me < n - 1)
    def _():
        held_up.wait_send()
        for it in range(ITERS):
            value_up[it].wait_send()

    for it in range(ITERS):
        everyone = square_in.at[it]
        pltpu.make_async_copy(everyone, everyone, square_send.at[it]).wait()
        for b in range(boards):
            pltpu.make_async_copy(reach.at[it, b], reach.at[it, b], reach_send.at[it, b]).wait()


def solution(mesh):
    n = mesh.shape["leaf"]

    def local(chance_reach, regrets_start, pot, parent, hand_cards, board_cards, hand_rank):
        leaf_rows, hands = chance_reach.shape[1:]
        boards = hand_rank.shape[0]
        rows = leaf_rows // boards
        leaf_count = parent.shape[1]
        width = round_up(hands, LANES)
        depth = round_up(DECK_SIZE + boards + 1, 16)
        chunks = boards + 2
        vmem = pl.BlockSpec(memory_space=pltpu.VMEM)
        shape = pltpu.VMEM(chance_reach.shape, F32)
        dma = pltpu.SemaphoreType.DMA
        arrays = (chance_reach, regrets_start, pot[None], parent, hand_cards.T, board_cards, hand_rank)
        return pl.pallas_call(
            functools.partial(kernel, n, boards, rows, hands, leaf_count),
            out_shape=(shape, shape),
            in_specs=[pl.BlockSpec(memory_space=pl.ANY)] * len(arrays),
            out_specs=(vmem, vmem),
            scratch_shapes=[
                *(pltpu.VMEM(array.shape, array.dtype) for array in arrays),
                pltpu.SemaphoreType.DMA((len(arrays),)),
                pltpu.VMEM((boards, width, width), BF16),
                pltpu.VMEM((depth, width), F32),
                pltpu.VMEM((depth, width + boards * LANES), BF16),
                pltpu.VMEM((boards, width), F32),
                pltpu.VMEM((2, width), jnp.int32),
                pltpu.VMEM((round_up(boards, 8), width), jnp.int32),
                pltpu.VMEM((boards, rows, LANES), F32),
                pltpu.VMEM((chunks * rows, 2 * chunks * rows), BF16),
                pltpu.VMEM((2 * rows, width), BF16),
                pltpu.VMEM((chunks, rows, hands), F32),
                pltpu.VMEM((ITERS, chunks * rows, hands), F32),
                pltpu.VMEM((ITERS, boards, rows, hands), F32),
                pltpu.VMEM((ITERS, boards, rows, hands), F32),
                pltpu.VMEM((ITERS, chunks, rows, hands), F32),
                pltpu.VMEM((ITERS, 1, LANES), F32),
                pltpu.VMEM((ITERS, n - 1, 1, LANES), F32),
                dma((2,)), dma((2,)),
                dma((ITERS, 2)), dma((ITERS, 2)),
                dma((ITERS, boards)), dma((ITERS, boards)),
                dma((ITERS,)), dma((ITERS,)),
            ],
            compiler_params=pltpu.CompilerParams(collective_id=0, has_side_effects=True),
            name="regret",
        )(*arrays)

    in_specs = (
        P("player", "leaf", None),
        P("player", "leaf", None),
        P("leaf"),
        P("player", None),
        P(),
        P("leaf", None),
        P("leaf", None),
    )
    out_specs = (P("player", "leaf", None), P("player", "leaf", None))
    return jax.shard_map(local, mesh=mesh, in_specs=in_specs, out_specs=out_specs, check_vma=False)
```

```python
import functools

import jax
import jax.numpy as jnp
from jax import lax
from jax.experimental import pallas as pl
from jax.experimental.pallas import tpu as pltpu
from jax.sharding import PartitionSpec as P

ITERS = 2
MOST = 6
DELTA = 0.05
EPSILON = 1e-06
DECK_SIZE = 52
LANES = 128
WIDE = 256
SPLIT = 3
MESH = pl.DeviceIdType.MESH
F32 = jnp.float32
BF16 = jnp.bfloat16


def round_up(value, unit):
    return (value + unit - 1) // unit * unit


def column_of(row, count):
    down = lax.broadcasted_iota(jnp.int32, (count, count), 0)
    across = lax.broadcasted_iota(jnp.int32, (count, count), 1)
    return jnp.sum(jnp.where(down == across, row, 0.0), axis=1, keepdims=True)


def row_of(column, count):
    down = lax.broadcasted_iota(jnp.int32, (count, count), 0)
    across = lax.broadcasted_iota(jnp.int32, (count, count), 1)
    return jnp.sum(jnp.where(down == across, column, 0.0), axis=0, keepdims=True)


def kernel(
    n, boards, rows, hands, leaf_count,
    chance_far, regrets_far, pot_far, parent_far, cards_far, board_cards_far, rank_far,
    out_regrets, out_values,
    chance, regrets, pot, parent, cards, board_cards, rank, load,
    payoff, left, right, free, cards_wide, rank_wide, pots, same, split,
    held, policy, reach, opposed, values, square_out, square_in,
    held_send, held_recv, value_send, value_recv, reach_send, reach_recv, square_send, square_recv,
):
    me = lax.axis_index("leaf")
    player = lax.axis_index("player")
    before, after = lax.rem(me + n - 1, n), lax.rem(me + 1, n)
    width = payoff.shape[1]
    depth = left.shape[0]
    chunks = boards + 2
    total = chunks * rows

    loads = [
        pltpu.make_async_copy(far, near, load.at[i])
        for i, (far, near) in enumerate((
            (cards_far, cards), (board_cards_far, board_cards), (rank_far, rank), (regrets_far, regrets),
            (pot_far, pot), (parent_far, parent), (chance_far, chance)))]
    for copy in loads:
        copy.start()

    zeros = jnp.zeros((rows, hands), F32)
    for edge in (0, chunks - 1):
        held[edge] = zeros
        for it in range(ITERS):
            values[it, edge] = zeros

    barrier = pltpu.get_barrier_semaphore()

    def greet(k, carry):
        pl.semaphore_signal(barrier, inc=1, device_id={"leaf": lax.rem(me + k, n)}, device_id_type=MESH)
        return carry

    pl.semaphore_signal(barrier, inc=1, device_id={"player": 1 - player}, device_id_type=MESH)
    lax.fori_loop(1, n, greet, 0)

    for copy in loads[:3]:
        copy.wait()

    cards_wide[...] = jnp.full(cards_wide.shape, -1, jnp.int32)
    cards_wide[:, :hands] = cards[...]
    rank_wide[...] = jnp.zeros(rank_wide.shape, jnp.int32)
    rank_wide[:boards, :hands] = rank[...]
    card = lax.broadcasted_iota(jnp.int32, (depth, width), 0)
    lane = lax.broadcasted_iota(jnp.int32, (depth, width), 1)
    holding = ((card == cards_wide[0:1, :]) | (card == cards_wide[1:2, :])).astype(F32)
    valid = ((card == depth - 1) & (lane < hands)).astype(F32)
    ranked = rank_wide[...]
    code = ((128 + (ranked & 127)) << (ranked >> 7)).astype(F32)
    left[...] = holding + valid
    left[DECK_SIZE : DECK_SIZE + boards, :] = code[:boards]
    right[:, :width] = (valid - holding).astype(BF16)
    pick = lax.broadcasted_iota(jnp.int32, (depth, boards * LANES), 0) - DECK_SIZE
    spot = lax.broadcasted_iota(jnp.int32, (depth, boards * LANES), 1)
    right[:, width:] = ((spot >= pick * LANES) & (spot < pick * LANES + LANES)).astype(BF16)
    deck = lax.broadcasted_iota(jnp.int32, (boards, depth), 1)
    on_board = jnp.zeros((boards, depth), jnp.bool_)
    for k in range(board_cards.shape[1]):
        on_board = on_board | (deck == board_cards[:, k : k + 1])
    touched = jnp.dot(on_board.astype(BF16), holding.astype(BF16), preferred_element_type=F32)
    free[...] = (touched < 0.5).astype(F32)

    def build(i, carry):
        start = pl.multiple_of(i * LANES, LANES)
        down = left[:, pl.ds(start, LANES)].T.astype(BF16)
        lows = jnp.dot(down, right[:, width:], preferred_element_type=F32).astype(BF16)
        for first in range(0, width, WIDE):
            last = min(first + WIDE, width)
            apart = jnp.dot(down, right[:, first:last], preferred_element_type=F32)
            apart = jnp.maximum(apart.astype(BF16), 0.0)
            for at in range(first, last, LANES):
                highs = [
                    jnp.broadcast_to(left[DECK_SIZE + b : DECK_SIZE + b + 1, at : at + LANES], (16, LANES)).astype(BF16)
                    for b in range(boards)]
                for r in range(0, LANES, 16):
                    bound = apart[r : r + 16, at - first : at - first + LANES]
                    floor = -bound
                    for b in range(boards):
                        gap = highs[b] - lows[r : r + 16, b * LANES : (b + 1) * LANES]
                        payoff[b, pl.ds(start + r, 16), at : at + LANES] = jnp.minimum(
                            jnp.maximum(gap, floor), bound)
        return carry

    blocks = width // LANES
    lax.fori_loop(0, SPLIT, build, 0)

    for copy in loads[3:]:
        copy.wait()
    pl.semaphore_wait(barrier, n)

    def to_before(source, target, send, recv):
        return pltpu.make_async_remote_copy(
            src_ref=source, dst_ref=target, send_sem=send, recv_sem=recv,
            device_id={"leaf": before}, device_id_type=MESH)

    def to_after(source, target, send, recv):
        return pltpu.make_async_remote_copy(
            src_ref=source, dst_ref=target, send_sem=send, recv_sem=recv,
            device_id={"leaf": after}, device_id_type=MESH)

    reach_of = min(MOST - 1, rows)
    held_down = to_before(
        regrets.at[0, pl.ds(0, reach_of)], held.at[chunks - 1, pl.ds(0, reach_of)], held_send.at[0], held_recv.at[0])
    held_up = to_after(
        regrets.at[0, pl.ds(boards * rows - reach_of, reach_of)], held.at[0, pl.ds(rows - reach_of, reach_of)], held_send.at[1], held_recv.at[1])
    value_down = [
        to_before(
            values.at[it, 1, pl.ds(0, reach_of)], values.at[it, chunks - 1, pl.ds(0, reach_of)], value_send.at[it, 0], value_recv.at[it, 0])
        for it in range(ITERS)]
    value_up = [
        to_after(
            values.at[it, boards, pl.ds(rows - reach_of, reach_of)], values.at[it, 0, pl.ds(rows - reach_of, reach_of)],
            value_send.at[it, 1], value_recv.at[it, 1])
        for it in range(ITERS)]

    @pl.when(me > 0)
    def _():
        held_down.start()

    @pl.when(me < n - 1)
    def _():
        held_up.start()

    twice = lax.broadcasted_iota(jnp.int32, (2 * total, leaf_count), 0)
    leaf = me * (boards * rows) - rows + jnp.where(twice >= total, twice - total, twice)
    here = lax.broadcasted_iota(jnp.int32, (2 * total, leaf_count), 1)
    ids = jnp.sum(jnp.where(leaf == here, parent[...].astype(F32) + 1.0, 0.0), axis=1, keepdims=True)
    same[...] = (ids[:total] == row_of(ids, 2 * total)).astype(BF16)
    pots[...] = jnp.broadcast_to(
        column_of(pot[...], boards * rows) * (1.0 / hands), (boards * rows, LANES)).reshape(boards, rows, LANES)
    split[...] = jnp.zeros(split.shape, BF16)
    for b in range(boards):
        held[b + 1] = regrets[0, pl.ds(b * rows, rows)]

    lax.fori_loop(SPLIT, blocks, build, 0)

    def node_totals(array):
        coarse = array.astype(BF16)
        fine = (array - coarse.astype(F32)).astype(BF16)
        return jnp.dot(same[...], jnp.concatenate([coarse, fine], axis=0), preferred_element_type=F32)

    @pl.when(me > 0)
    def _():
        held_up.wait_recv()

    @pl.when(me < n - 1)
    def _():
        held_down.wait_recv()

    standing = held[...].reshape(total, hands)
    for it in range(ITERS):
        positive = jnp.maximum(standing, 0.0) + DELTA
        policy[it] = positive / node_totals(positive)
        own_policy = policy[it, rows : rows + boards * rows]
        reach[it] = (chance[0] * own_policy).reshape(boards, rows, hands)

        def exchange(b, it=it):
            return pltpu.make_async_remote_copy(
                src_ref=reach.at[it, b], dst_ref=opposed.at[it, b],
                send_sem=reach_send.at[it, b], recv_sem=reach_recv.at[it, b],
                device_id={"player": 1 - player}, device_id_type=MESH)

        for t in range(boards):
            exchange(t * (boards - 1) % boards).start()

        def showdown(t, carry, it=it, exchange=exchange):
            b = lax.rem(t * (boards - 1), boards)
            exchange(b).wait_recv()
            open_hands = free[pl.ds(b, 1), :]
            facing = opposed[it, b] * open_hands[:, :hands]
            coarse = facing.astype(BF16).astype(F32)
            split[:, :hands] = jnp.concatenate([coarse, facing - coarse], axis=0).astype(BF16)
            summed = jnp.dot(split[...], payoff[b], preferred_element_type=F32)
            summed = (summed[:rows] + summed[rows:]) * open_hands * pots[b][:, :1]
            values[it, b + 1] = summed[:, :hands]

            @pl.when((t == 0) & (me > 0))
            def _():
                value_down[it].start()

            @pl.when((t == 1) & (me < n - 1))
            def _():
                value_up[it].start()

            return carry

        lax.fori_loop(0, boards, showdown, 0)

        @pl.when(me > 0)
        def _(it=it):
            value_up[it].wait_recv()

        @pl.when(me < n - 1)
        def _(it=it):
            value_down[it].wait_recv()

        gained = values[it].reshape(total, hands)
        instant = gained - node_totals(policy[it] * gained)
        own = instant[rows : rows + boards * rows]
        squares = jnp.sum(jnp.sum(own * own, axis=0, keepdims=True), axis=1, keepdims=True)
        square_out[it] = jnp.broadcast_to(squares, (1, LANES))

        def tell(k, carry, it=it):
            pltpu.make_async_remote_copy(
                src_ref=square_out.at[it], dst_ref=square_in.at[it, k - 1],
                send_sem=square_send.at[it], recv_sem=square_recv.at[it],
                device_id={"leaf": lax.rem(me + k, n)}, device_id_type=MESH).start()
            return carry

        lax.fori_loop(1, n, tell, 0)
        if it == ITERS - 1:
            out_values[0] = gained[rows : rows + boards * rows]
        everyone = square_in.at[it]
        pltpu.make_async_copy(everyone, everyone, square_recv.at[it]).wait()
        squares = square_out[it] + jnp.sum(square_in[it], axis=0)
        inverse = 1.0 / jnp.sqrt(squares[:, :1] / (leaf_count * hands) + EPSILON)
        if it < ITERS - 1:
            standing = standing + instant * inverse
        else:
            out_regrets[0] = standing[rows : rows + boards * rows] + own * inverse

    @pl.when(me > 0)
    def _():
        held_down.wait_send()
        for it in range(ITERS):
            value_down[it].wait_send()

    @pl.when(me < n - 1)
    def _():
        held_up.wait_send()
        for it in range(ITERS):
            value_up[it].wait_send()

    for it in range(ITERS):
        everyone = square_in.at[it]
        pltpu.make_async_copy(everyone, everyone, square_send.at[it]).wait()
        for b in range(boards):
            pltpu.make_async_copy(reach.at[it, b], reach.at[it, b], reach_send.at[it, b]).wait()


def solution(mesh):
    n = mesh.shape["leaf"]

    def local(chance_reach, regrets_start, pot, parent, hand_cards, board_cards, hand_rank):
        leaf_rows, hands = chance_reach.shape[1:]
        boards = hand_rank.shape[0]
        rows = leaf_rows // boards
        leaf_count = parent.shape[1]
        width = round_up(hands, LANES)
        depth = round_up(DECK_SIZE + boards + 1, 16)
        chunks = boards + 2
        vmem = pl.BlockSpec(memory_space=pltpu.VMEM)
        shape = pltpu.VMEM(chance_reach.shape, F32)
        dma = pltpu.SemaphoreType.DMA
        arrays = (chance_reach, regrets_start, pot[None], parent, hand_cards.T, board_cards, hand_rank)
        return pl.pallas_call(
            functools.partial(kernel, n, boards, rows, hands, leaf_count),
            out_shape=(shape, shape),
            in_specs=[pl.BlockSpec(memory_space=pl.ANY)] * len(arrays),
            out_specs=(vmem, vmem),
            scratch_shapes=[
                *(pltpu.VMEM(array.shape, array.dtype) for array in arrays),
                pltpu.SemaphoreType.DMA((len(arrays),)),
                pltpu.VMEM((boards, width, width), BF16),
                pltpu.VMEM((depth, width), F32),
                pltpu.VMEM((depth, width + boards * LANES), BF16),
                pltpu.VMEM((boards, width), F32),
                pltpu.VMEM((2, width), jnp.int32),
                pltpu.VMEM((round_up(boards, 8), width), jnp.int32),
                pltpu.VMEM((boards, rows, LANES), F32),
                pltpu.VMEM((chunks * rows, 2 * chunks * rows), BF16),
                pltpu.VMEM((2 * rows, width), BF16),
                pltpu.VMEM((chunks, rows, hands), F32),
                pltpu.VMEM((ITERS, chunks * rows, hands), F32),
                pltpu.VMEM((ITERS, boards, rows, hands), F32),
                pltpu.VMEM((ITERS, boards, rows, hands), F32),
                pltpu.VMEM((ITERS, chunks, rows, hands), F32),
                pltpu.VMEM((ITERS, 1, LANES), F32),
                pltpu.VMEM((ITERS, n - 1, 1, LANES), F32),
                dma((2,)), dma((2,)),
                dma((ITERS, 2)), dma((ITERS, 2)),
                dma((ITERS, boards)), dma((ITERS, boards)),
                dma((ITERS,)), dma((ITERS,)),
            ],
            compiler_params=pltpu.CompilerParams(collective_id=0, has_side_effects=True),
            name="regret",
        )(*arrays)

    in_specs = (
        P("player", "leaf", None),
        P("player", "leaf", None),
        P("leaf"),
        P("player", None),
        P(),
        P("leaf", None),
        P("leaf", None),
    )
    out_specs = (P("player", "leaf", None), P("player", "leaf", None))
    return jax.shard_map(local, mesh=mesh, in_specs=in_specs, out_specs=out_specs, check_vma=False)
```
